32 devices in a mesh: lon: 4 (over y, x), lat: 8 (over z, core).
Axes of the slice: x: 2, y: 2, z: 4, core: 2. Of those that a mesh axis runs over, the one named last changes fastest.
Arguments:
- spectrum: float32 [32, 512, 648], P('lon', 'lat'), may hold values from 0.01 to 1
- sea_mask: int32 [32, 512], P('lon', 'lat'), may hold values from 0 to 1, as said below
- ice_flags: int32 [32, 512], P('lon', 'lat'), may hold values 0 or 1
- wind_forcing: float32 [32, 512], P('lon', 'lat'), may hold values from 0.1 to 1.5
- group_speed: float32 [18], replicated, may hold values from 0.3 to 1
- coupling: bfloat16 [648, 648], replicated, may hold values from -0.25 to 0.25
Outputs:
- field: float32 [32, 512, 648], P('lon', 'lat')
The draws below stay inside these ranges and needn't reach their ends.
Inputs may be any that keep to these rules, and one draw needn't show every extreme that they name: `sea_mask`: each device's block of 8 x 64 cells holds at most 384 sea cells and at least 128; in every draw some block holds exactly 384.
All inputs are finite; a program needn't handle non-finite values. No bound on the sum of `ice_flags` on one device may be relied on, other than what follows from the above.
Results may differ from the reference program's by a relative error of at most 0.00079.
Values sent between devices are 32-bit elements; how exact they have to be, the bound alone decides.
A program may use at most 64 MiB of HBM per device.

```python
import math
import jax
import jax.numpy as jnp

DIRS = 36
FREQS = 18
BINS = 648
CX = 8
CY = 64
SEA_DEV = 384
STEPS = 4
NX = 32
NY = 512


def draw_sea_mask(key, part):
    blocks_x = NX // CX
    blocks_y = NY // CY
    cells = CX * CY
    blocks = blocks_x * blocks_y
    key_count, key_pick, key_order = jax.random.split(jax.random.fold_in(key, 11), 3)
    counts = jax.random.randint(key_count, (blocks,), SEA_DEV // 3, SEA_DEV + 1)
    chosen = jax.random.randint(key_pick, (), 0, blocks)
    counts = counts.at[chosen].set(SEA_DEV)
    scores = jax.random.randint(key_order, (blocks, cells), 0, 2 ** 20) * cells + jnp.arange(cells, dtype=jnp.int32)[None, :]
    order = jnp.argsort(scores, axis=1, stable=True)
    ranks = jnp.argsort(order, axis=1, stable=True)
    flags = (ranks < counts[:, None]).astype(jnp.int32)
    flags = flags.reshape(blocks_x, blocks_y, CX, CY).transpose(0, 2, 1, 3)
    return flags.reshape(NX, NY)


def set_ends(array, key, low, largest):
    dims = array.shape
    index_at = [jax.random.randint(jax.random.fold_in(key, axis), (), 0, dims[axis]) for axis in range(len(dims))]
    array = array.at[tuple(index_at)].set(low)
    longest = dims.index(max(dims))
    index_at[longest] = (index_at[longest] + 1) % dims[longest]
    return array.at[tuple(index_at)].set(largest)


def levels(key, shape, cuts, least, largest):
    gain = 1.0
    for dim, parts in cuts:
        heights = jax.random.uniform(jax.random.fold_in(jax.random.fold_in(key, 6), dim), (parts,), jnp.float32, least / len(cuts), largest / len(cuts))
        gain = gain * jnp.repeat(jnp.exp(heights), shape[dim] // parts).reshape((-1,) + (1,) * (len(shape) - 1 - dim))
    return gain


def noise(stream_key, extent, scale, limit, kind=jnp.bfloat16):
    return jnp.clip(scale * jax.random.normal(stream_key, extent, jnp.float32), -limit, limit).astype(kind)


def setup_inputs(seed: int = 0) -> dict:
    arg_keys = jax.random.split(jax.random.key(seed), 7)
    spectrum = jnp.clip(jnp.exp(math.log(1.0) - 4.6051702 * jax.random.uniform(arg_keys[0], (NX, NY, BINS), jnp.float32) ** levels(arg_keys[0], (NX, NY, BINS), ((0, 4), (1, 8)), -0.2, 0.2)), 0.01, 1.0)
    sea_mask = draw_sea_mask(jax.random.fold_in(arg_keys[6], 71), 0)
    ice_flags = set_ends((jax.random.randint(arg_keys[2], (NX, NY), 0, 4) < 1).astype(jnp.int32), jax.random.fold_in(arg_keys[2], 1), 0, 1)
    wind_forcing = jnp.clip(jnp.exp(math.log(1.5) - 2.7080502 * jax.random.uniform(arg_keys[3], (NX, NY), jnp.float32) ** levels(arg_keys[3], (NX, NY), ((0, 4), (1, 8)), -0.2, 0.2)), 0.1, 1.5)
    group_speed = jnp.clip(jax.random.uniform(arg_keys[4], (FREQS,), jnp.float32, 0.3, 1.0), 0.3, 1.0)
    coupling = noise(arg_keys[5], (BINS, BINS), BINS ** -0.5, 0.25)
    return {"spectrum": spectrum, "sea_mask": sea_mask, "ice_flags": ice_flags, "wind_forcing": wind_forcing, "group_speed": group_speed, "coupling": coupling}


time_step = 0.2
dissipation = 0.5


def speed_tables(rows, total_rows, group_speed, dirs):
    theta = (jnp.arange(dirs).astype(jnp.float32) + 0.5) * (2.0 * math.pi / dirs)
    latitude = (-60.0 + 120.0 * (rows.astype(jnp.float32) + 0.5) / total_rows) * (math.pi / 180.0)
    scaled = jnp.outer(jnp.cos(theta), group_speed).reshape(-1)
    along_x = (0.225 * scaled)[None, :] / jnp.cos(latitude)[:, None]
    along_y = 0.45 * jnp.outer(jnp.sin(theta), group_speed).reshape(-1)
    return along_x, along_y


def upwind(field, west, east, south, north, along_x, along_y):
    speed_x = along_x[None]
    result = field - jnp.maximum(speed_x, 0.0) * (field - west) - jnp.minimum(speed_x, 0.0) * (east - field)
    return result - jnp.maximum(along_y, 0.0) * (field - south) - jnp.minimum(along_y, 0.0) * (north - field)


def sources(advected, wind_forcing, ice_flags, coupling):
    shape = advected.shape
    energy = jnp.mean(advected, axis=-1, keepdims=True)
    flat = advected.reshape(-1, shape[-1]).astype(jnp.bfloat16)
    transfer = jnp.dot(flat, coupling, preferred_element_type=jnp.float32).reshape(shape)
    forcing = (wind_forcing * (1.0 - ice_flags.astype(jnp.float32)))[..., None]
    return advected + time_step * (forcing * advected + transfer - dissipation * energy * advected)


def reference(spectrum, sea_mask, ice_flags, wind_forcing, group_speed, coupling):
    sea = sea_mask.astype(jnp.float32)[..., None]
    along_x, along_y = speed_tables(jnp.arange(NY), NY, group_speed, DIRS)
    field = spectrum * sea
    for step in range(STEPS):
        west = jnp.roll(field, 1, axis=0)
        east = jnp.roll(field, -1, axis=0)
        edge = jnp.zeros_like(field[:, :1])
        south = jnp.concatenate([edge, field[:, :-1]], axis=1)
        north = jnp.concatenate([field[:, 1:], edge], axis=1)
        advected = upwind(field, west, east, south, north, along_x, along_y)
        field = sources(advected, wind_forcing, ice_flags, coupling) * sea
    return field
```

```python
import functools
import math

import jax
import jax.numpy as jnp
from jax import lax
from jax.experimental import pallas as pl
from jax.experimental.pallas import tpu as pltpu
from jax.sharding import PartitionSpec as P

DIRS = 36
STEPS = 4
LANES = 128
PAD = 8
CHUNKS = 2
SHIFT = 40
MESH = pl.DeviceIdType.MESH

time_step = 0.2
dissipation = 0.5


def kernel(
    freqs, speed_ref, sea_ref, ice_ref, wind_ref, spectrum_ref, coupling_ref, out_ref,
    field, staged, weights, raw_weights, rounded, keep_x, push_x, push_y, grow, scale,
    east_out, east_in, west_out, west_in, north_out, north_in, south_out, south_in,
    load_sem, weight_sem, store_sem, lon_send, lon_recv, lat_send, lat_recv,
):
    columns, rows, bins = staged.shape
    tiles = field.shape[2]
    piece = rows // CHUNKS
    mean_of = 1.0 / bins
    quarter, half, late = DIRS // 4 * freqs, DIRS // 2 * freqs, DIRS * 3 // 4 * freqs
    cut_w, cut_y, cut_e = quarter - LANES, half - 2 * LANES, late - 3 * LANES
    tail = bins - (tiles - 1) * LANES

    lon, lat = lax.axis_index("lon"), lax.axis_index("lat")
    lons, lats = lax.axis_size("lon"), lax.axis_size("lat")
    east, west = lax.rem(lon + 1, lons), lax.rem(lon + lons - 1, lons)
    has_south, has_north = lat > 0, lat < lats - 1

    def width(t):
        return LANES if t < tiles - 1 else tail

    order = [0, columns - 1] + list(range(1, columns - 1))
    loads = {
        c: pltpu.make_async_copy(spectrum_ref.at[c], staged.at[c], load_sem.at[c]) for c in order
    }
    for c in order:
        loads[c].start()
    weight_load = pltpu.make_async_copy(coupling_ref, raw_weights, weight_sem)
    weight_load.start()

    barrier = pltpu.get_barrier_semaphore()
    pl.semaphore_signal(barrier, inc=1, device_id=(east, lat), device_id_type=MESH)
    pl.semaphore_signal(barrier, inc=1, device_id=(west, lat), device_id_type=MESH)

    @pl.when(has_south)
    def _():
        pl.semaphore_signal(barrier, inc=1, device_id=(lon, lat - 1), device_id_type=MESH)

    @pl.when(has_north)
    def _():
        pl.semaphore_signal(barrier, inc=1, device_id=(lon, lat + 1), device_id_type=MESH)

    sea = sea_ref[...].astype(jnp.float32)
    forcing = wind_ref[...] * (1.0 - ice_ref[...].astype(jnp.float32))
    growth = jnp.transpose(sea * (1.0 + time_step * forcing))
    sea_rows = jnp.transpose(sea)
    for c in range(columns):
        grow[c] = jnp.broadcast_to(growth[:, c : c + 1], (rows, LANES))
        scale[c] = jnp.broadcast_to(sea_rows[:, c : c + 1], (rows, LANES))

    lane = lax.broadcasted_iota(jnp.int32, (8, LANES), 1)
    lane_piece = lax.broadcasted_iota(jnp.int32, (piece, LANES), 1)
    row = lax.broadcasted_iota(jnp.int32, (rows, LANES), 0) + lat * rows
    latitude = (-60.0 + 120.0 * (row.astype(jnp.float32) + 0.5) / (rows * lats)) * (math.pi / 180.0)
    inverse = 1.0 / jnp.cos(latitude)
    for t in range(tiles):
        number = (lane + t * LANES).astype(jnp.float32)
        direction = jnp.floor((number + 0.5) * (1.0 / freqs))
        freq = number - direction * freqs
        speed = jnp.zeros((8, LANES), jnp.float32)
        for f in range(freqs):
            speed = jnp.where(freq == f, speed_ref[f], speed)
        inside = (lane + t * LANES) < bins
        theta = (direction + 0.5) * (2.0 * math.pi / DIRS)
        along_y = jnp.where(inside, jnp.abs(0.45 * jnp.sin(theta) * speed), 0.0)
        along_x = jnp.where(inside, jnp.abs(0.225 * jnp.cos(theta) * speed), 0.0)
        push_y[t] = along_y
        along_x = along_x[0:1] * inverse
        push_x[t] = along_x
        keep_x[t] = 1.0 - along_x - along_y[0:1]

    zero_row = jnp.zeros((1, LANES), jnp.float32)
    for c in range(columns):
        for t in range(tiles):
            for b in range(2):
                field[b, c, t, PAD - 1 : PAD, :] = zero_row
                field[b, c, t, PAD + rows : PAD + rows + 1, :] = zero_row
        field[0, c, tiles - 1, PAD : PAD + rows, :] = jnp.zeros((rows, LANES), jnp.float32)

    def lon_copy(step, side, k):
        span = pl.ds(k * piece, piece)
        out_buf, in_buf, to = ((east_out, west_in, east), (west_out, east_in, west))[side]
        return pltpu.make_async_remote_copy(
            src_ref=out_buf.at[step, :, span, :],
            dst_ref=in_buf.at[step, :, span, :],
            send_sem=lon_send.at[step, side, k],
            recv_sem=lon_recv.at[step, side, k],
            device_id=(to, lat),
            device_id_type=MESH,
        )

    def lat_copy(step, side):
        out_buf, in_buf, to = ((north_out, south_in, lat + 1), (south_out, north_in, lat - 1))[side]
        return pltpu.make_async_remote_copy(
            src_ref=out_buf.at[step],
            dst_ref=in_buf.at[step],
            send_sem=lat_send.at[step, side],
            recv_sem=lat_recv.at[step, side],
            device_id=(lon, to),
            device_id_type=MESH,
        )

    def send_lon(step, k):
        b = step % 2
        span = slice(k * piece, (k + 1) * piece)
        at = slice(PAD + k * piece, PAD + (k + 1) * piece)
        last = columns - 1
        east_out[step, 0, span, :] = field[b, last, 0, at, :]
        end = pltpu.roll(field[b, last, 5, at, :], SHIFT, 1)
        mixed = jnp.where(lane_piece < cut_w, field[b, last, 1, at, :], end)
        east_out[step, 1, span, :] = jnp.where(lane_piece < cut_e, mixed, field[b, last, 3, at, :])
        east_out[step, 2, span, :] = field[b, last, 4, at, :]
        for i in range(3):
            west_out[step, i, span, :] = field[b, 0, i + 1, at, :]
        lon_copy(step, 0, k).start()
        lon_copy(step, 1, k).start()

    def send_north(step):
        b = step % 2
        low = lane[0:1] < cut_y
        edge = slice(PAD + rows - 1, PAD + rows)
        for c in range(columns):
            for i in range(3):
                north_out[step, i, c : c + 1, :] = field[b, c, i, edge, :]

        @pl.when(has_north)
        def _():
            lat_copy(step, 0).start()

    def send_south(step):
        b = step % 2
        low = lane[0:1] < cut_y
        edge = slice(PAD, PAD + 1)
        for c in range(columns):
            south_out[step, 0, c : c + 1, :] = jnp.where(
                low, field[b, c, 5, edge, :], field[b, c, 2, edge, :]
            )
            for i in range(1, 3):
                south_out[step, i, c : c + 1, :] = field[b, c, i + 2, edge, :]

        @pl.when(has_south)
        def _():
            lat_copy(step, 1).start()

    def take_south(step):
        b = step % 2

        @pl.when(has_south)
        def _():
            lat_copy(step, 0).wait_recv()
            for c in range(columns):
                for i in range(3):
                    field[b, c, i, PAD - 1 : PAD, :] = south_in[step, i, c : c + 1, :]

    def take_north(step):
        b = step % 2
        edge = slice(PAD + rows, PAD + rows + 1)

        @pl.when(has_north)
        def _():
            lat_copy(step, 1).wait_recv()
            for c in range(columns):
                for i, t in ((0, 2), (1, 3), (2, 4), (0, 5)):
                    field[b, c, t, edge, :] = north_in[step, i, c : c + 1, :]

    def advance(step, k, group):
        b = step % 2
        at = slice(PAD + k * piece, PAD + (k + 1) * piece)
        up = slice(at.start - 1, at.stop - 1)
        down = slice(at.start + 1, at.stop + 1)
        span = slice(k * piece, (k + 1) * piece)
        first = group[0]

        def from_west(c, t):
            if c > 0:
                return field[b, c - 1, t, at, :]
            value = west_in[step, {0: 0, 1: 1, 3: 1, 4: 2, 5: 1}[t], span, :]
            return pltpu.roll(value, LANES - SHIFT, 1) if t == 5 else value

        def from_east(c, t):
            if c < columns - 1:
                return field[b, c + 1, t, at, :]
            return east_in[step, t - 1, span, :]

        totals = []
        for n, c in enumerate(group):
            total = None
            for t in range(tiles):
                if t == 1:
                    beside = jnp.where(lane_piece < cut_w, from_west(c, t), from_east(c, t))
                elif t == 2:
                    beside = from_east(c, t)
                elif t == 3:
                    beside = jnp.where(lane_piece < cut_e, from_east(c, t), from_west(c, t))
                else:
                    beside = from_west(c, t)
                if t < 2:
                    along = field[b, c, t, up, :]
                elif t == 2:
                    along = jnp.where(lane_piece < cut_y, field[b, c, t, up, :], field[b, c, t, down, :])
                else:
                    along = field[b, c, t, down, :]
                advected = (
                    keep_x[t, span, :] * field[b, c, t, at, :]
                    + push_x[t, span, :] * beside
                    + push_y[t, 0:1, :] * along
                )
                field[1 - b, c, t, at, :] = advected
                rounded[n * piece : (n + 1) * piece, t * LANES : (t + 1) * LANES] = advected.astype(
                    jnp.bfloat16
                )
                total = advected if total is None else total + advected
            energy = jnp.sum(total, axis=1, keepdims=True) * mean_of
            sea_here = scale[c, span, :]
            totals.append(grow[c, span, :] - (time_step * dissipation) * energy * sea_here)
        size = len(group) * piece
        transfer = jnp.dot(rounded[0:size, :], weights[...], preferred_element_type=jnp.float32)
        for n, c in enumerate(group):
            sea_here = time_step * scale[c, span, :]
            for t in range(tiles):
                moved = transfer[n * piece : (n + 1) * piece, t * LANES : (t + 1) * LANES]
                value = totals[n] * field[1 - b, c, t, at, :] + sea_here * moved
                if step < STEPS - 1:
                    field[1 - b, c, t, at, :] = value
                else:
                    w = width(t)
                    staged[c, span, t * LANES : t * LANES + w] = value[:, 0:w]

    heard = 2 + has_south.astype(jnp.int32) + has_north.astype(jnp.int32)
    pl.semaphore_wait(barrier, heard)

    for n, c in enumerate(order):
        loads[c].wait()
        for t in range(tiles):
            w = width(t)
            field[0, c, t, PAD : PAD + rows, 0:w] = (
                staged[c, :, t * LANES : t * LANES + w] * scale[c, :, 0:w]
            )
        if n == 1:
            for k in range(CHUNKS):
                send_lon(0, k)
    send_north(0)
    send_south(0)

    weight_load.wait()
    weights[...] = jnp.zeros_like(weights)
    weights[0:bins, 0:bins] = raw_weights[...]

    edges, inner = [0, columns - 1], list(range(1, columns - 1))
    stores = []
    for step in range(STEPS):
        for k in range(CHUNKS):
            if k == 0:
                take_south(step)
            if k == CHUNKS - 1:
                take_north(step)
            for side in range(2):
                lon_copy(step, side, k).wait_recv()
            advance(step, k, edges)
            if step < STEPS - 1:
                send_lon(step + 1, k)
            advance(step, k, inner)
            if step < STEPS - 1:
                if k == 0:
                    send_south(step + 1)
                if k == CHUNKS - 1:
                    send_north(step + 1)
            else:
                span = pl.ds(k * piece, piece)
                store = pltpu.make_async_copy(
                    staged.at[:, span, :], out_ref.at[:, span, :], store_sem.at[k]
                )
                store.start()
                stores.append(store)
    for store in stores:
        store.wait()
    for step in range(STEPS):
        for k in range(CHUNKS):
            for side in range(2):
                lon_copy(step, side, k).wait_send()

        @pl.when(has_north)
        def _():
            lat_copy(step, 0).wait_send()

        @pl.when(has_south)
        def _():
            lat_copy(step, 1).wait_send()


def on_device(spectrum, sea_mask, ice_flags, wind_forcing, group_speed, coupling):
    columns, rows, bins = spectrum.shape
    tiles = -(-bins // LANES)
    wide = tiles * LANES
    piece = rows // CHUNKS
    vmem = pl.BlockSpec(memory_space=pltpu.VMEM)
    anywhere = pl.BlockSpec(memory_space=pl.ANY)
    f32 = jnp.float32
    lon_buffer = pltpu.VMEM((STEPS, 3, rows, LANES), f32)
    lat_buffer = pltpu.VMEM((STEPS, 3, columns, LANES), f32)
    return pl.pallas_call(
        functools.partial(kernel, group_speed.shape[0]),
        out_shape=jax.ShapeDtypeStruct(spectrum.shape, spectrum.dtype),
        in_specs=[pl.BlockSpec(memory_space=pltpu.SMEM), vmem, vmem, vmem, anywhere, anywhere],
        out_specs=anywhere,
        scratch_shapes=[
            pltpu.VMEM((2, columns, tiles, rows + 2 * PAD, LANES), f32),
            pltpu.VMEM((columns, rows, bins), f32),
            pltpu.VMEM((wide, wide), jnp.bfloat16),
            pltpu.VMEM((bins, bins), jnp.bfloat16),
            pltpu.VMEM(((columns - 2) * piece, wide), jnp.bfloat16),
            pltpu.VMEM((tiles, rows, LANES), f32),
            pltpu.VMEM((tiles, rows, LANES), f32),
            pltpu.VMEM((tiles, 8, LANES), f32),
            pltpu.VMEM((columns, rows, LANES), f32),
            pltpu.VMEM((columns, rows, LANES), f32),
            lon_buffer, lon_buffer, lon_buffer, lon_buffer,
            lat_buffer, lat_buffer, lat_buffer, lat_buffer,
            pltpu.SemaphoreType.DMA((columns,)),
            pltpu.SemaphoreType.DMA,
            pltpu.SemaphoreType.DMA((CHUNKS,)),
            pltpu.SemaphoreType.DMA((STEPS, 2, CHUNKS)),
            pltpu.SemaphoreType.DMA((STEPS, 2, CHUNKS)),
            pltpu.SemaphoreType.DMA((STEPS, 2)),
            pltpu.SemaphoreType.DMA((STEPS, 2)),
        ],
        compiler_params=pltpu.CompilerParams(
            collective_id=0, has_side_effects=True, vmem_limit_bytes=48 * 1024 * 1024
        ),
    )(group_speed, sea_mask, ice_flags, wind_forcing, spectrum, coupling)


def solution(mesh):
    placed = (P("lon", "lat", None), P("lon", "lat"), P("lon", "lat"), P("lon", "lat"), P(), P())
    return jax.shard_map(
        on_device, mesh=mesh, in_specs=placed, out_specs=P("lon", "lat", None), check_vma=False
    )
```

```python
import functools
import math

import jax
import jax.numpy as jnp
from jax import lax
from jax.experimental import pallas as pl
from jax.experimental.pallas import tpu as pltpu
from jax.sharding import PartitionSpec as P

DIRS = 36
STEPS = 4
LANES = 128
PAD = 8
CHUNKS = 4
SHIFT = 40
MESH = pl.DeviceIdType.MESH

time_step = 0.2
dissipation = 0.5


def kernel(
    freqs, speed_hbm, sea_hbm, ice_hbm, wind_hbm, spectrum_ref, coupling_ref, out_ref,
    speed_ref, sea_ref, ice_ref, wind_ref,
    field, staged, weights, raw_weights, rounded, keep_x, push_x, push_y, grow, scale,
    east_out, east_in, west_out, west_in, north_out, north_in, south_out, south_in,
    load_sem, small_sem, weight_sem, store_sem, lon_send, lon_recv, lat_send, lat_recv,
):
    columns, rows, bins = staged.shape
    tiles = field.shape[2]
    piece = rows // CHUNKS
    mean_of = 1.0 / bins
    quarter, half, late = DIRS // 4 * freqs, DIRS // 2 * freqs, DIRS * 3 // 4 * freqs
    cut_w, cut_y, cut_e = quarter - LANES, half - 2 * LANES, late - 3 * LANES
    tail = bins - (tiles - 1) * LANES

    lon, lat = lax.axis_index("lon"), lax.axis_index("lat")
    lons, lats = lax.axis_size("lon"), lax.axis_size("lat")
    east, west = lax.rem(lon + 1, lons), lax.rem(lon + lons - 1, lons)
    has_south, has_north = lat > 0, lat < lats - 1

    def width(t):
        return LANES if t < tiles - 1 else tail

    order = [0, columns - 1] + list(range(1, columns - 1))
    loads = {
        c: pltpu.make_async_copy(spectrum_ref.at[c], staged.at[c], load_sem.at[c]) for c in order
    }
    small = [
        pltpu.make_async_copy(source, target, small_sem.at[n])
        for n, (source, target) in enumerate(
            ((speed_hbm, speed_ref), (sea_hbm, sea_ref), (ice_hbm, ice_ref), (wind_hbm, wind_ref))
        )
    ]
    for copy in small:
        copy.start()
    for c in order:
        loads[c].start()
    weight_load = pltpu.make_async_copy(coupling_ref, raw_weights, weight_sem)
    weight_load.start()

    barrier = pltpu.get_barrier_semaphore()
    pl.semaphore_signal(barrier, inc=1, device_id=(east, lat), device_id_type=MESH)
    pl.semaphore_signal(barrier, inc=1, device_id=(west, lat), device_id_type=MESH)

    @pl.when(has_south)
    def _():
        pl.semaphore_signal(barrier, inc=1, device_id=(lon, lat - 1), device_id_type=MESH)

    @pl.when(has_north)
    def _():
        pl.semaphore_signal(barrier, inc=1, device_id=(lon, lat + 1), device_id_type=MESH)

    for copy in small:
        copy.wait()
    sea = sea_ref[...].astype(jnp.float32)
    forcing = wind_ref[...] * (1.0 - ice_ref[...].astype(jnp.float32))
    growth = jnp.transpose(sea * (1.0 + time_step * forcing))
    sea_rows = jnp.transpose(sea)
    for c in range(columns):
        grow[c] = jnp.broadcast_to(growth[:, c : c + 1], (rows, LANES))
        scale[c] = jnp.broadcast_to(sea_rows[:, c : c + 1], (rows, LANES))

    lane = lax.broadcasted_iota(jnp.int32, (8, LANES), 1)
    lane_piece = lax.broadcasted_iota(jnp.int32, (piece, LANES), 1)
    row = lax.broadcasted_iota(jnp.int32, (rows, LANES), 0) + lat * rows
    latitude = (-60.0 + 120.0 * (row.astype(jnp.float32) + 0.5) / (rows * lats)) * (math.pi / 180.0)
    inverse = 1.0 / jnp.cos(latitude)
    for t in range(tiles):
        number = (lane + t * LANES).astype(jnp.float32)
        direction = jnp.floor((number + 0.5) * (1.0 / freqs))
        freq = number - direction * freqs
        speed = jnp.zeros((8, LANES), jnp.float32)
        for f in range(freqs):
            speed = jnp.where(freq == f, speed_ref[f], speed)
        inside = (lane + t * LANES) < bins
        theta = (direction + 0.5) * (2.0 * math.pi / DIRS)
        along_y = jnp.where(inside, jnp.abs(0.45 * jnp.sin(theta) * speed), 0.0)
        along_x = jnp.where(inside, jnp.abs(0.225 * jnp.cos(theta) * speed), 0.0)
        push_y[t] = along_y
        along_x = along_x[0:1] * inverse
        push_x[t] = along_x
        keep_x[t] = 1.0 - along_x - along_y[0:1]

    zero_row = jnp.zeros((1, LANES), jnp.float32)
    for c in range(columns):
        for t in range(tiles):
            for b in range(2):
                field[b, c, t, PAD - 1 : PAD, :] = zero_row
                field[b, c, t, PAD + rows : PAD + rows + 1, :] = zero_row
        field[0, c, tiles - 1, PAD : PAD + rows, :] = jnp.zeros((rows, LANES), jnp.float32)

    def lon_copy(step, side, k):
        span = pl.ds(k * piece, piece)
        out_buf, in_buf, to = ((east_out, west_in, east), (west_out, east_in, west))[side]
        return pltpu.make_async_remote_copy(
            src_ref=out_buf.at[step, :, span, :],
            dst_ref=in_buf.at[step, :, span, :],
            send_sem=lon_send.at[step, side, k],
            recv_sem=lon_recv.at[step, side, k],
            device_id=(to, lat),
            device_id_type=MESH,
        )

    def lat_copy(step, side):
        out_buf, in_buf, to = ((north_out, south_in, lat + 1), (south_out, north_in, lat - 1))[side]
        return pltpu.make_async_remote_copy(
            src_ref=out_buf.at[step],
            dst_ref=in_buf.at[step],
            send_sem=lat_send.at[step, side],
            recv_sem=lat_recv.at[step, side],
            device_id=(lon, to),
            device_id_type=MESH,
        )

    def send_lon(step, k):
        b = step % 2
        span = slice(k * piece, (k + 1) * piece)
        at = slice(PAD + k * piece, PAD + (k + 1) * piece)
        last = columns - 1
        east_out[step, 0, span, :] = field[b, last, 0, at, :]
        end = pltpu.roll(field[b, last, 5, at, :], SHIFT, 1)
        mixed = jnp.where(lane_piece < cut_w, field[b, last, 1, at, :], end)
        east_out[step, 1, span, :] = jnp.where(lane_piece < cut_e, mixed, field[b, last, 3, at, :])
        east_out[step, 2, span, :] = field[b, last, 4, at, :]
        for i in range(3):
            west_out[step, i, span, :] = field[b, 0, i + 1, at, :]
        lon_copy(step, 0, k).start()
        lon_copy(step, 1, k).start()

    def send_north(step):
        b = step % 2
        low = lane[0:1] < cut_y
        edge = slice(PAD + rows - 1, PAD + rows)
        for c in range(columns):
            for i in range(3):
                north_out[step, i, c : c + 1, :] = field[b, c, i, edge, :]

        @pl.when(has_north)
        def _():
            lat_copy(step, 0).start()

    def send_south(step):
        b = step % 2
        low = lane[0:1] < cut_y
        edge = slice(PAD, PAD + 1)
        for c in range(columns):
            south_out[step, 0, c : c + 1, :] = jnp.where(
                low, field[b, c, 5, edge, :], field[b, c, 2, edge, :]
            )
            for i in range(1, 3):
                south_out[step, i, c : c + 1, :] = field[b, c, i + 2, edge, :]

        @pl.when(has_south)
        def _():
            lat_copy(step, 1).start()

    def take_south(step):
        b = step % 2

        @pl.when(has_south)
        def _():
            lat_copy(step, 0).wait_recv()
            for c in range(columns):
                for i in range(3):
                    field[b, c, i, PAD - 1 : PAD, :] = south_in[step, i, c : c + 1, :]

    def take_north(step):
        b = step % 2
        edge = slice(PAD + rows, PAD + rows + 1)

        @pl.when(has_north)
        def _():
            lat_copy(step, 1).wait_recv()
            for c in range(columns):
                for i, t in ((0, 2), (1, 3), (2, 4), (0, 5)):
                    field[b, c, t, edge, :] = north_in[step, i, c : c + 1, :]

    def advance(step, k, group):
        b = step % 2
        at = slice(PAD + k * piece, PAD + (k + 1) * piece)
        up = slice(at.start - 1, at.stop - 1)
        down = slice(at.start + 1, at.stop + 1)
        span = slice(k * piece, (k + 1) * piece)
        first = group[0]

        def from_west(c, t):
            if c > 0:
                return field[b, c - 1, t, at, :]
            value = west_in[step, {0: 0, 1: 1, 3: 1, 4: 2, 5: 1}[t], span, :]
            return pltpu.roll(value, LANES - SHIFT, 1) if t == 5 else value

        def from_east(c, t):
            if c < columns - 1:
                return field[b, c + 1, t, at, :]
            return east_in[step, t - 1, span, :]

        totals = []
        for n, c in enumerate(group):
            total = None
            for t in range(tiles):
                if t == 1:
                    beside = jnp.where(lane_piece < cut_w, from_west(c, t), from_east(c, t))
                elif t == 2:
                    beside = from_east(c, t)
                elif t == 3:
                    beside = jnp.where(lane_piece < cut_e, from_east(c, t), from_west(c, t))
                else:
                    beside = from_west(c, t)
                if t < 2:
                    along = field[b, c, t, up, :]
                elif t == 2:
                    along = jnp.where(lane_piece < cut_y, field[b, c, t, up, :], field[b, c, t, down, :])
                else:
                    along = field[b, c, t, down, :]
                advected = (
                    keep_x[t, span, :] * field[b, c, t, at, :]
                    + push_x[t, span, :] * beside
                    + push_y[t, 0:1, :] * along
                )
                field[1 - b, c, t, at, :] = advected
                rounded[n * piece : (n + 1) * piece, t * LANES : (t + 1) * LANES] = advected.astype(
                    jnp.bfloat16
                )
                total = advected if total is None else total + advected
            energy = jnp.sum(total, axis=1, keepdims=True) * mean_of
            sea_here = scale[c, span, :]
            totals.append(grow[c, span, :] - (time_step * dissipation) * energy * sea_here)
        size = len(group) * piece
        transfer = jnp.dot(rounded[0:size, :], weights[...], preferred_element_type=jnp.float32)
        for n, c in enumerate(group):
            sea_here = time_step * scale[c, span, :]
            for t in range(tiles):
                moved = transfer[n * piece : (n + 1) * piece, t * LANES : (t + 1) * LANES]
                value = totals[n] * field[1 - b, c, t, at, :] + sea_here * moved
                if step < STEPS - 1:
                    field[1 - b, c, t, at, :] = value
                else:
                    w = width(t)
                    staged[c, span, t * LANES : t * LANES + w] = value[:, 0:w]

    heard = 2 + has_south.astype(jnp.int32) + has_north.astype(jnp.int32)
    pl.semaphore_wait(barrier, heard)

    for n, c in enumerate(order):
        loads[c].wait()
        for t in range(tiles):
            w = width(t)
            field[0, c, t, PAD : PAD + rows, 0:w] = (
                staged[c, :, t * LANES : t * LANES + w] * scale[c, :, 0:w]
            )
        if n == 1:
            for k in range(CHUNKS):
                send_lon(0, k)
    send_north(0)
    send_south(0)

    weight_load.wait()
    weights[...] = jnp.zeros_like(weights)
    weights[0:bins, 0:bins] = raw_weights[...]

    edges, inner = [0, columns - 1], list(range(1, columns - 1))
    stores = []
    for step in range(STEPS):
        for k in range(CHUNKS):
            if k == 0:
                take_south(step)
            if k == CHUNKS - 1:
                take_north(step)
            for side in range(2):
                lon_copy(step, side, k).wait_recv()
            advance(step, k, edges)
            if step < STEPS - 1:
                send_lon(step + 1, k)
            advance(step, k, inner)
            if step < STEPS - 1:
                if k == 0:
                    send_south(step + 1)
                if k == CHUNKS - 1:
                    send_north(step + 1)
            else:
                span = pl.ds(k * piece, piece)
                store = pltpu.make_async_copy(
                    staged.at[:, span, :], out_ref.at[:, span, :], store_sem.at[k]
                )
                store.start()
                stores.append(store)
    for store in stores:
        store.wait()
    for step in range(STEPS):
        for k in range(CHUNKS):
            for side in range(2):
                lon_copy(step, side, k).wait_send()

        @pl.when(has_north)
        def _():
            lat_copy(step, 0).wait_send()

        @pl.when(has_south)
        def _():
            lat_copy(step, 1).wait_send()


def on_device(spectrum, sea_mask, ice_flags, wind_forcing, group_speed, coupling):
    columns, rows, bins = spectrum.shape
    tiles = -(-bins // LANES)
    wide = tiles * LANES
    piece = rows // CHUNKS
    hbm = pl.BlockSpec(memory_space=pltpu.HBM)
    anywhere = pl.BlockSpec(memory_space=pl.ANY)
    f32 = jnp.float32
    lon_buffer = pltpu.VMEM((STEPS, 3, rows, LANES), f32)
    lat_buffer = pltpu.VMEM((STEPS, 3, columns, LANES), f32)
    return pl.pallas_call(
        functools.partial(kernel, group_speed.shape[0]),
        out_shape=jax.ShapeDtypeStruct(spectrum.shape, spectrum.dtype),
        in_specs=[hbm] * 6,
        out_specs=anywhere,
        scratch_shapes=[
            pltpu.SMEM(group_speed.shape, f32),
            pltpu.VMEM((columns, rows), jnp.int32),
            pltpu.VMEM((columns, rows), jnp.int32),
            pltpu.VMEM((columns, rows), f32),
            pltpu.VMEM((2, columns, tiles, rows + 2 * PAD, LANES), f32),
            pltpu.VMEM((columns, rows, bins), f32),
            pltpu.VMEM((wide, wide), jnp.bfloat16),
            pltpu.VMEM((bins, bins), jnp.bfloat16),
            pltpu.VMEM(((columns - 2) * piece, wide), jnp.bfloat16),
            pltpu.VMEM((tiles, rows, LANES), f32),
            pltpu.VMEM((tiles, rows, LANES), f32),
            pltpu.VMEM((tiles, 8, LANES), f32),
            pltpu.VMEM((columns, rows, LANES), f32),
            pltpu.VMEM((columns, rows, LANES), f32),
            lon_buffer, lon_buffer, lon_buffer, lon_buffer,
            lat_buffer, lat_buffer, lat_buffer, lat_buffer,
            pltpu.SemaphoreType.DMA((columns,)),
            pltpu.SemaphoreType.DMA((4,)),
            pltpu.SemaphoreType.DMA,
            pltpu.SemaphoreType.DMA((CHUNKS,)),
            pltpu.SemaphoreType.DMA((STEPS, 2, CHUNKS)),
            pltpu.SemaphoreType.DMA((STEPS, 2, CHUNKS)),
            pltpu.SemaphoreType.DMA((STEPS, 2)),
            pltpu.SemaphoreType.DMA((STEPS, 2)),
        ],
        compiler_params=pltpu.CompilerParams(
            collective_id=0, has_side_effects=True, vmem_limit_bytes=60 * 1024 * 1024
        ),
    )(group_speed, sea_mask, ice_flags, wind_forcing, spectrum, coupling)


def solution(mesh):
    placed = (P("lon", "lat", None), P("lon", "lat"), P("lon", "lat"), P("lon", "lat"), P(), P())
    return jax.shard_map(
        on_device, mesh=mesh, in_specs=placed, out_specs=P("lon", "lat", None), check_vma=False
    )
```

```python
import functools
import math

import jax
import jax.numpy as jnp
from jax import lax
from jax.experimental import pallas as pl
from jax.experimental.pallas import tpu as pltpu
from jax.sharding import PartitionSpec as P

DIRS = 36
STEPS = 4
LANES = 128
PAD = 8
CHUNKS = 4
MESH = pl.DeviceIdType.MESH

time_step = 0.2
dissipation = 0.5


def kernel(
    freqs, speed_hbm, sea_hbm, ice_hbm, wind_hbm, spectrum_ref, coupling_ref, out_ref,
    speed_ref, sea_ref, ice_ref, wind_ref,
    field, staged, weights, raw_weights, rounded, keep_x, push_x, push_y, grow, scale,
    east_out, east_in, west_out, west_in, north_out, north_in, south_out, south_in,
    load_sem, small_sem, weight_sem, lon_send, lon_recv, lat_send, lat_recv,
):
    columns, rows, bins = staged.shape
    tiles = field.shape[2]
    piece = rows // CHUNKS
    mean_of = 1.0 / bins
    quarter, half, late = DIRS // 4 * freqs, DIRS // 2 * freqs, DIRS * 3 // 4 * freqs
    cut_w, cut_y, cut_e = quarter - LANES, half - 2 * LANES, late - 3 * LANES
    late_w = LANES - cut_e
    tail = bins - (tiles - 1) * LANES

    lon, lat = lax.axis_index("lon"), lax.axis_index("lat")
    lons, lats = lax.axis_size("lon"), lax.axis_size("lat")
    east, west = lax.rem(lon + 1, lons), lax.rem(lon + lons - 1, lons)
    has_south, has_north = lat > 0, lat < lats - 1

    def width(t):
        return LANES if t < tiles - 1 else tail

    last = columns - 1
    edges, inner = [0, last], list(range(1, last))
    loads = [
        pltpu.make_async_copy(spectrum_ref.at[c], staged.at[c], load_sem.at[c])
        for c in range(columns)
    ]
    weight_load = pltpu.make_async_copy(coupling_ref, raw_weights, weight_sem)
    small = [
        pltpu.make_async_copy(source, target, small_sem.at[n])
        for n, (source, target) in enumerate(
            ((sea_hbm, sea_ref), (speed_hbm, speed_ref), (ice_hbm, ice_ref), (wind_hbm, wind_ref))
        )
    ]
    for copy in small:
        copy.start()
    for c in edges:
        loads[c].start()

    barrier = pltpu.get_barrier_semaphore()
    pl.semaphore_signal(barrier, inc=1, device_id=(east, lat), device_id_type=MESH)
    pl.semaphore_signal(barrier, inc=1, device_id=(west, lat), device_id_type=MESH)

    @pl.when(has_south)
    def _():
        pl.semaphore_signal(barrier, inc=1, device_id=(lon, lat - 1), device_id_type=MESH)

    @pl.when(has_north)
    def _():
        pl.semaphore_signal(barrier, inc=1, device_id=(lon, lat + 1), device_id_type=MESH)

    small[0].wait()
    sea = sea_ref[...].astype(jnp.float32)
    sea_rows = jnp.transpose(sea)
    for c in range(columns):
        scale[c] = jnp.broadcast_to(sea_rows[:, c : c + 1], (rows, LANES))

    lane = lax.broadcasted_iota(jnp.int32, (8, LANES), 1)
    lane_piece = lax.broadcasted_iota(jnp.int32, (piece, LANES), 1)
    lane_eight = lax.broadcasted_iota(jnp.int32, (8, LANES), 1)
    row_eight = lax.broadcasted_iota(jnp.int32, (8, LANES), 0)
    own_low = lane_eight // 4 == row_eight
    own_high = lane_eight // 4 == row_eight + 8
    low_half = lane_eight < LANES // 2

    def pack(buffer, loose):
        upper, lower = loose[0:8], loose[8:16]
        buffer[32:40, :] = jnp.where(low_half, upper, pltpu.roll(lower, 64, 1))
        spread = jnp.where(own_low, pltpu.roll(upper, 64, 1, stride=4, stride_axis=0), 0.0)
        spread += jnp.where(own_high, pltpu.roll(lower, 96, 1, stride=4, stride_axis=0), 0.0)
        buffer[40:41, :] = jnp.sum(spread, axis=0, keepdims=True)

    def unpack(buffer):
        main = buffer[32:40, :]
        rest = jnp.broadcast_to(buffer[40:41, :], (8, LANES))
        rest = pltpu.roll(rest, 64, 1)
        for bit in range(3):
            moved = pltpu.roll(rest, LANES - 4 * 2**bit, 1)
            rest = jnp.where(row_eight // 2**bit % 2 == 1, moved, rest)
        upper = jnp.where(low_half, main, rest)
        lower = jnp.where(low_half, pltpu.roll(main, 64, 1), pltpu.roll(rest, 96, 1))
        return jnp.concatenate([upper, lower], axis=0)

    def lon_copy(step, side, k):
        out_buf, in_buf, to = ((east_out, west_in, east), (west_out, east_in, west))[side]
        return pltpu.make_async_remote_copy(
            src_ref=out_buf.at[step, k],
            dst_ref=in_buf.at[step, k],
            send_sem=lon_send.at[step, side, k],
            recv_sem=lon_recv.at[step, side, k],
            device_id=(to, lat),
            device_id_type=MESH,
        )

    def lat_copy(step, side):
        out_buf, in_buf, to = ((north_out, south_in, lat + 1), (south_out, north_in, lat - 1))[side]
        return pltpu.make_async_remote_copy(
            src_ref=out_buf.at[step],
            dst_ref=in_buf.at[step],
            send_sem=lat_send.at[step, side],
            recv_sem=lat_recv.at[step, side],
            device_id=(lon, to),
            device_id_type=MESH,
        )

    def send_lon(step, k):
        b = step % 2
        at = slice(PAD + k * piece, PAD + (k + 1) * piece)
        buffer = east_out.at[step, k]
        buffer[0:16, :] = field[b, last, 0, at, :]
        buffer[16:32, :] = field[b, last, 4, at, :]
        loose = jnp.where(
            lane_piece < cut_w + late_w,
            pltpu.roll(field[b, last, 1, at, :], late_w, 1),
            pltpu.roll(field[b, last, 5, at, :], cut_w + late_w, 1),
        )
        pack(
            buffer,
            jnp.where(lane_piece < late_w, pltpu.roll(field[b, last, 3, at, :], late_w, 1), loose),
        )
        buffer = west_out.at[step, k]
        first_part = field[b, 0, 1, at, :]
        buffer[0:16, :] = field[b, 0, 2, at, :]
        buffer[16:32, :] = jnp.where(lane_piece < cut_e, field[b, 0, 3, at, :], first_part)
        pack(buffer, pltpu.roll(first_part, LANES - cut_w, 1))
        lon_copy(step, 0, k).start()
        lon_copy(step, 1, k).start()

    def send_north(step):
        b = step % 2
        low = lane[0:1] < cut_y
        edge = slice(PAD + rows - 1, PAD + rows)
        for c in range(columns):
            for i in range(3):
                north_out[step, i, c : c + 1, :] = field[b, c, i, edge, :]

        @pl.when(has_north)
        def _():
            lat_copy(step, 0).start()

    def send_south(step):
        b = step % 2
        low = lane[0:1] < cut_y
        edge = slice(PAD, PAD + 1)
        for c in range(columns):
            south_out[step, 0, c : c + 1, :] = jnp.where(
                low, field[b, c, 5, edge, :], field[b, c, 2, edge, :]
            )
            for i in range(1, 3):
                south_out[step, i, c : c + 1, :] = field[b, c, i + 2, edge, :]

        @pl.when(has_south)
        def _():
            lat_copy(step, 1).start()

    def take_south(step):
        b = step % 2

        @pl.when(has_south)
        def _():
            lat_copy(step, 0).wait_recv()
            for c in range(columns):
                for i in range(3):
                    field[b, c, i, PAD - 1 : PAD, :] = south_in[step, i, c : c + 1, :]

    def take_north(step):
        b = step % 2
        edge = slice(PAD + rows, PAD + rows + 1)

        @pl.when(has_north)
        def _():
            lat_copy(step, 1).wait_recv()
            for c in range(columns):
                for i, t in ((0, 2), (1, 3), (2, 4), (0, 5)):
                    field[b, c, t, edge, :] = north_in[step, i, c : c + 1, :]

    def advance(step, k, group):
        b = step % 2
        at = slice(PAD + k * piece, PAD + (k + 1) * piece)
        up = slice(at.start - 1, at.stop - 1)
        down = slice(at.start + 1, at.stop + 1)
        span = slice(k * piece, (k + 1) * piece)
        if 0 in group:
            buffer = west_in.at[step, k]
            loose = unpack(buffer)
            shared = pltpu.roll(loose, LANES - late_w, 1)
            west_halo = {
                0: buffer[0:16, :],
                1: shared,
                3: shared,
                4: buffer[16:32, :],
                5: pltpu.roll(loose, LANES - cut_w - late_w, 1),
            }
        if last in group:
            buffer = east_in.at[step, k]
            shared = buffer[16:32, :]
            moved = pltpu.roll(unpack(buffer), cut_w, 1)
            east_halo = {
                1: jnp.where(lane_piece < cut_e, moved, shared), 2: buffer[0:16, :], 3: shared
            }

        def from_west(c, t):
            return field[b, c - 1, t, at, :] if c > 0 else west_halo[t]

        def from_east(c, t):
            return field[b, c + 1, t, at, :] if c < last else east_halo[t]

        totals = []
        for n, c in enumerate(group):
            total = None
            for t in range(tiles):
                if t == 1:
                    beside = jnp.where(lane_piece < cut_w, from_west(c, t), from_east(c, t))
                elif t == 2:
                    beside = from_east(c, t)
                elif t == 3:
                    beside = jnp.where(lane_piece < cut_e, from_east(c, t), from_west(c, t))
                else:
                    beside = from_west(c, t)
                if t < 2:
                    along = field[b, c, t, up, :]
                elif t == 2:
                    along = jnp.where(lane_piece < cut_y, field[b, c, t, up, :], field[b, c, t, down, :])
                else:
                    along = field[b, c, t, down, :]
                advected = (
                    keep_x[t, span, :] * field[b, c, t, at, :]
                    + push_x[t, span, :] * beside
                    + push_y[t, 0:1, :] * along
                )
                field[1 - b, c, t, at, :] = advected
                rounded[n * piece : (n + 1) * piece, t * LANES : (t + 1) * LANES] = advected.astype(
                    jnp.bfloat16
                )
                total = advected if total is None else total + advected
            energy = jnp.sum(total, axis=1, keepdims=True) * mean_of
            sea_here = scale[c, span, :]
            totals.append(grow[c, span, :] - (time_step * dissipation) * energy * sea_here)
        size = len(group) * piece
        transfer = jnp.dot(rounded[0:size, :], weights[...], preferred_element_type=jnp.float32)
        for n, c in enumerate(group):
            sea_here = time_step * scale[c, span, :]
            for t in range(tiles):
                moved = transfer[n * piece : (n + 1) * piece, t * LANES : (t + 1) * LANES]
                value = totals[n] * field[1 - b, c, t, at, :] + sea_here * moved
                if step < STEPS - 1:
                    field[1 - b, c, t, at, :] = value
                else:
                    w = width(t)
                    out_ref[c, span, t * LANES : t * LANES + w] = value[:, 0:w]

    heard = 2 + has_south.astype(jnp.int32) + has_north.astype(jnp.int32)
    pl.semaphore_wait(barrier, heard)

    def take_column(c):
        for t in range(tiles):
            w = width(t)
            field[0, c, t, PAD : PAD + rows, 0:w] = (
                staged[c, :, t * LANES : t * LANES + w] * scale[c, :, 0:w]
            )

    for c in edges:
        field[0, c, tiles - 1, PAD : PAD + rows, :] = jnp.zeros((rows, LANES), jnp.float32)
    for c in edges:
        loads[c].wait()
    for c in inner:
        loads[c].start()
    weight_load.start()
    for c in edges:
        take_column(c)
    for k in range(CHUNKS):
        send_lon(0, k)

    for copy in small[1:]:
        copy.wait()
    forcing = wind_ref[...] * (1.0 - ice_ref[...].astype(jnp.float32))
    growth = jnp.transpose(sea * (1.0 + time_step * forcing))
    for c in range(columns):
        grow[c] = jnp.broadcast_to(growth[:, c : c + 1], (rows, LANES))
    row = lax.broadcasted_iota(jnp.int32, (rows, LANES), 0) + lat * rows
    latitude = (-60.0 + 120.0 * (row.astype(jnp.float32) + 0.5) / (rows * lats)) * (math.pi / 180.0)
    inverse = 1.0 / jnp.cos(latitude)
    for t in range(tiles):
        number = (lane + t * LANES).astype(jnp.float32)
        direction = jnp.floor((number + 0.5) * (1.0 / freqs))
        freq = number - direction * freqs
        speed = jnp.zeros((8, LANES), jnp.float32)
        for f in range(freqs):
            speed = jnp.where(freq == f, speed_ref[f], speed)
        inside = (lane + t * LANES) < bins
        theta = (direction + 0.5) * (2.0 * math.pi / DIRS)
        along_y = jnp.where(inside, jnp.abs(0.45 * jnp.sin(theta) * speed), 0.0)
        along_x = jnp.where(inside, jnp.abs(0.225 * jnp.cos(theta) * speed), 0.0)
        push_y[t] = along_y
        along_x = along_x[0:1] * inverse
        push_x[t] = along_x
        keep_x[t] = 1.0 - along_x - along_y[0:1]

    zero_row = jnp.zeros((1, LANES), jnp.float32)
    for c in range(columns):
        for t in range(tiles):
            for b in range(2):
                field[b, c, t, PAD - 1 : PAD, :] = zero_row
                field[b, c, t, PAD + rows : PAD + rows + 1, :] = zero_row
        if c in inner:
            field[0, c, tiles - 1, PAD : PAD + rows, :] = jnp.zeros((rows, LANES), jnp.float32)

    for c in inner:
        loads[c].wait()
        take_column(c)
    send_north(0)
    send_south(0)

    weight_load.wait()
    weights[...] = jnp.zeros_like(weights)
    weights[0:bins, 0:bins] = raw_weights[...]

    for step in range(STEPS - 1):
        for k in range(CHUNKS):
            if k == 0:
                take_south(step)
            if k == CHUNKS - 1:
                take_north(step)
            for side in range(2):
                lon_copy(step, side, k).wait_recv()
            advance(step, k, edges)
            send_lon(step + 1, k)
            advance(step, k, inner)
            if k == 0:
                send_south(step + 1)
            if k == CHUNKS - 1:
                send_north(step + 1)
    take_south(STEPS - 1)
    take_north(STEPS - 1)
    for k in range(CHUNKS):
        advance(STEPS - 1, k, inner)
    for k in range(CHUNKS):
        for side in range(2):
            lon_copy(STEPS - 1, side, k).wait_recv()
        advance(STEPS - 1, k, edges)
    for step in range(STEPS):
        for k in range(CHUNKS):
            for side in range(2):
                lon_copy(step, side, k).wait_send()

        @pl.when(has_north)
        def _():
            lat_copy(step, 0).wait_send()

        @pl.when(has_south)
        def _():
            lat_copy(step, 1).wait_send()


def on_device(spectrum, sea_mask, ice_flags, wind_forcing, group_speed, coupling):
    columns, rows, bins = spectrum.shape
    tiles = -(-bins // LANES)
    wide = tiles * LANES
    piece = rows // CHUNKS
    hbm = pl.BlockSpec(memory_space=pltpu.HBM)
    operands = (group_speed, sea_mask, ice_flags, wind_forcing, spectrum, coupling)
    f32 = jnp.float32
    lon_buffer = pltpu.VMEM((STEPS, CHUNKS, 41, LANES), f32)
    lat_buffer = pltpu.VMEM((STEPS, 3, columns, LANES), f32)
    return pl.pallas_call(
        functools.partial(kernel, group_speed.shape[0]),
        out_shape=jax.ShapeDtypeStruct(spectrum.shape, spectrum.dtype),
        in_specs=[hbm] * 6,
        out_specs=pl.BlockSpec(memory_space=pltpu.VMEM),
        scratch_shapes=[
            pltpu.SMEM(group_speed.shape, f32),
            pltpu.VMEM((columns, rows), jnp.int32),
            pltpu.VMEM((columns, rows), jnp.int32),
            pltpu.VMEM((columns, rows), f32),
            pltpu.VMEM((2, columns, tiles, rows + 2 * PAD, LANES), f32),
            pltpu.VMEM((columns, rows, bins), f32),
            pltpu.VMEM((wide, wide), jnp.bfloat16),
            pltpu.VMEM((bins, bins), jnp.bfloat16),
            pltpu.VMEM(((columns - 2) * piece, wide), jnp.bfloat16),
            pltpu.VMEM((tiles, rows, LANES), f32),
            pltpu.VMEM((tiles, rows, LANES), f32),
            pltpu.VMEM((tiles, 8, LANES), f32),
            pltpu.VMEM((columns, rows, LANES), f32),
            pltpu.VMEM((columns, rows, LANES), f32),
            lon_buffer, lon_buffer, lon_buffer, lon_buffer,
            lat_buffer, lat_buffer, lat_buffer, lat_buffer,
            pltpu.SemaphoreType.DMA((columns,)),
            pltpu.SemaphoreType.DMA((4,)),
            pltpu.SemaphoreType.DMA,
            pltpu.SemaphoreType.DMA((STEPS, 2, CHUNKS)),
            pltpu.SemaphoreType.DMA((STEPS, 2, CHUNKS)),
            pltpu.SemaphoreType.DMA((STEPS, 2)),
            pltpu.SemaphoreType.DMA((STEPS, 2)),
        ],
        compiler_params=pltpu.CompilerParams(
            collective_id=0, has_side_effects=True, vmem_limit_bytes=32 * 1024 * 1024
        ),
    )(*(pltpu.with_memory_space_constraint(x, pltpu.HBM) for x in operands))


def solution(mesh):
    placed = (P("lon", "lat", None), P("lon", "lat"), P("lon", "lat"), P("lon", "lat"), P(), P())
    return jax.shard_map(
        on_device, mesh=mesh, in_specs=placed, out_specs=P("lon", "lat", None), check_vma=False
    )
```

```python
import functools
import math

import jax
import jax.numpy as jnp
from jax import lax
from jax.experimental import pallas as pl
from jax.experimental.pallas import tpu as pltpu
from jax.sharding import PartitionSpec as P

DIRS = 36
STEPS = 4
LANES = 128
PAD = 8
CHUNKS = 4
MESH = pl.DeviceIdType.MESH

time_step = 0.2
dissipation = 0.5


def kernel(
    freqs, speed_hbm, sea_hbm, ice_hbm, wind_hbm, spectrum_ref, coupling_ref, out_ref,
    speed_ref, sea_ref, ice_ref, wind_ref,
    field, staged, weights, raw_weights, rounded, keep_x, push_x, push_y, grow, scale,
    east_out, east_in, west_out, west_in, north_out, north_in, south_out, south_in,
    load_sem, small_sem, weight_sem, lon_send, lon_recv, lat_send, lat_recv,
):
    columns, rows, bins = staged.shape
    tiles = field.shape[2]
    piece = rows // CHUNKS
    mean_of = 1.0 / bins
    quarter, half, late = DIRS // 4 * freqs, DIRS // 2 * freqs, DIRS * 3 // 4 * freqs
    cut_w, cut_y, cut_e = quarter - LANES, half - 2 * LANES, late - 3 * LANES
    late_w = LANES - cut_e
    tail = bins - (tiles - 1) * LANES

    lon, lat = lax.axis_index("lon"), lax.axis_index("lat")
    lons, lats = lax.axis_size("lon"), lax.axis_size("lat")
    east, west = lax.rem(lon + 1, lons), lax.rem(lon + lons - 1, lons)
    has_south, has_north = lat > 0, lat < lats - 1

    def width(t):
        return LANES if t < tiles - 1 else tail

    last = columns - 1
    edges, inner = [0, last], list(range(1, last))
    loads = [
        pltpu.make_async_copy(spectrum_ref.at[c], staged.at[c], load_sem.at[c])
        for c in range(columns)
    ]
    weight_load = pltpu.make_async_copy(coupling_ref, raw_weights, weight_sem)
    small = [
        pltpu.make_async_copy(source, target, small_sem.at[n])
        for n, (source, target) in enumerate(
            ((sea_hbm, sea_ref), (speed_hbm, speed_ref), (ice_hbm, ice_ref), (wind_hbm, wind_ref))
        )
    ]
    for copy in small:
        copy.start()
    for c in edges:
        loads[c].start()

    barrier = pltpu.get_barrier_semaphore()
    pl.semaphore_signal(barrier, inc=1, device_id=(east, lat), device_id_type=MESH)
    pl.semaphore_signal(barrier, inc=1, device_id=(west, lat), device_id_type=MESH)

    @pl.when(has_south)
    def _():
        pl.semaphore_signal(barrier, inc=1, device_id=(lon, lat - 1), device_id_type=MESH)

    @pl.when(has_north)
    def _():
        pl.semaphore_signal(barrier, inc=1, device_id=(lon, lat + 1), device_id_type=MESH)

    small[0].wait()
    sea = sea_ref[...].astype(jnp.float32)
    sea_rows = jnp.transpose(sea)
    for c in range(columns):
        scale[c] = jnp.broadcast_to(sea_rows[:, c : c + 1], (rows, LANES))

    lane = lax.broadcasted_iota(jnp.int32, (8, LANES), 1)
    lane_piece = lax.broadcasted_iota(jnp.int32, (piece, LANES), 1)
    lane_eight = lax.broadcasted_iota(jnp.int32, (8, LANES), 1)
    row_eight = lax.broadcasted_iota(jnp.int32, (8, LANES), 0)
    own_low = lane_eight // 4 == row_eight + 1
    own_high = lane_eight // 4 == row_eight + 9
    low_half = lane_eight < LANES // 2

    def turn(value, by):
        return pltpu.roll(value, by % LANES, 1)

    def gather_rest(upper, lower, start):
        base = (4 - start) % LANES
        up = pltpu.roll(upper, base, 1, stride=4, stride_axis=0)
        down = pltpu.roll(lower, base + 32, 1, stride=4, stride_axis=0)
        spread = jnp.where(own_low, up, 0.0) + jnp.where(own_high, down, 0.0)
        return jnp.sum(spread, axis=0, keepdims=True)

    def spread_rest(line, start):
        line = jnp.broadcast_to(line, (8, LANES))
        halves = []
        for part in range(2):
            value = turn(line, start - 4 - 32 * part)
            for i in range(1, 8):
                value = jnp.where(row_eight == i, turn(line, start - 4 - 4 * i - 32 * part), value)
            halves.append(value)
        return halves

    def lon_copy(step, side, k):
        out_buf, in_buf, to = ((east_out, west_in, east), (west_out, east_in, west))[side]
        return pltpu.make_async_remote_copy(
            src_ref=out_buf.at[step, k],
            dst_ref=in_buf.at[step, k],
            send_sem=lon_send.at[step, side, k],
            recv_sem=lon_recv.at[step, side, k],
            device_id=(to, lat),
            device_id_type=MESH,
        )

    def lat_copy(step, side):
        out_buf, in_buf, to = ((north_out, south_in, lat + 1), (south_out, north_in, lat - 1))[side]
        return pltpu.make_async_remote_copy(
            src_ref=out_buf.at[step],
            dst_ref=in_buf.at[step],
            send_sem=lat_send.at[step, side],
            recv_sem=lat_recv.at[step, side],
            device_id=(lon, to),
            device_id_type=MESH,
        )

    def send_lon(step, k):
        b = step % 2
        at = slice(PAD + k * piece, PAD + (k + 1) * piece)
        buffer = east_out.at[step, k]
        buffer[0:16, :] = field[b, last, 0, at, :]
        buffer[16:32, :] = field[b, last, 4, at, :]
        ends = []
        for part in range(2):
            rows_at = slice(at.start + 8 * part, at.start + 8 * part + 8)
            move, offset = late_w + 64 * part, lane_eight - 64 * part
            value = jnp.where(
                offset < cut_w + late_w,
                turn(field[b, last, 1, rows_at, :], move),
                turn(field[b, last, 5, rows_at, :], move + cut_w),
            )
            ends.append(
                jnp.where(offset < late_w, turn(field[b, last, 3, rows_at, :], move), value)
            )
        buffer[32:40, :] = jnp.where(low_half, ends[0], ends[1])
        buffer[40:41, :] = gather_rest(
            field[b, last, 5, at.start : at.start + 8, :], field[b, last, 5, at.start + 8 : at.stop, :],
            64 - late_w - cut_w,
        )
        buffer = west_out.at[step, k]
        first_part = field[b, 0, 1, at, :]
        buffer[0:16, :] = field[b, 0, 2, at, :]
        buffer[16:32, :] = jnp.where(lane_piece < cut_e, field[b, 0, 3, at, :], first_part)
        buffer[32:40, :] = jnp.where(
            low_half, turn(first_part[0:8], -cut_w), turn(first_part[8:16], 64 - cut_w)
        )
        buffer[40:41, :] = gather_rest(first_part[0:8], first_part[8:16], 64 + cut_w)
        lon_copy(step, 0, k).start()
        lon_copy(step, 1, k).start()

    def send_north(step):
        b = step % 2
        low = lane[0:1] < cut_y
        edge = slice(PAD + rows - 1, PAD + rows)
        for c in range(columns):
            for i in range(3):
                north_out[step, i, c : c + 1, :] = field[b, c, i, edge, :]

        @pl.when(has_north)
        def _():
            lat_copy(step, 0).start()

    def send_south(step):
        b = step % 2
        low = lane[0:1] < cut_y
        edge = slice(PAD, PAD + 1)
        for c in range(columns):
            south_out[step, 0, c : c + 1, :] = jnp.where(
                low, field[b, c, 5, edge, :], field[b, c, 2, edge, :]
            )
            for i in range(1, 3):
                south_out[step, i, c : c + 1, :] = field[b, c, i + 2, edge, :]

        @pl.when(has_south)
        def _():
            lat_copy(step, 1).start()

    def take_south(step):
        b = step % 2

        @pl.when(has_south)
        def _():
            lat_copy(step, 0).wait_recv()
            for c in range(columns):
                for i in range(3):
                    field[b, c, i, PAD - 1 : PAD, :] = south_in[step, i, c : c + 1, :]

    def take_north(step):
        b = step % 2
        edge = slice(PAD + rows, PAD + rows + 1)

        @pl.when(has_north)
        def _():
            lat_copy(step, 1).wait_recv()
            for c in range(columns):
                for i, t in ((0, 2), (1, 3), (2, 4), (0, 5)):
                    field[b, c, t, edge, :] = north_in[step, i, c : c + 1, :]

    def advance(step, k, group):
        b = step % 2
        at = slice(PAD + k * piece, PAD + (k + 1) * piece)
        up = slice(at.start - 1, at.stop - 1)
        down = slice(at.start + 1, at.stop + 1)
        span = slice(k * piece, (k + 1) * piece)
        if 0 in group:
            buffer = west_in.at[step, k]
            main, inside = buffer[32:40, :], 64 - late_w - cut_w
            rest = spread_rest(buffer[40:41, :], inside)
            shared = jnp.concatenate([turn(main, -late_w), turn(main, 64 - late_w)], axis=0)
            ends = [
                jnp.where(lane_eight < inside, turn(main, 64 * part + inside - 64), rest[part])
                for part in range(2)
            ]
            west_halo = {
                0: buffer[0:16, :],
                1: shared,
                3: shared,
                4: buffer[16:32, :],
                5: jnp.concatenate(ends, axis=0),
            }
        if last in group:
            buffer = east_in.at[step, k]
            main, shared = buffer[32:40, :], buffer[16:32, :]
            rest = spread_rest(buffer[40:41, :], 64 + cut_w)
            moved = [
                jnp.where(lane_eight < 64 + cut_w, turn(main, cut_w - 64 * part), rest[part])
                for part in range(2)
            ]
            moved = jnp.concatenate(moved, axis=0)
            east_halo = {
                1: jnp.where(lane_piece < cut_e, moved, shared), 2: buffer[0:16, :], 3: shared
            }

        def from_west(c, t):
            return field[b, c - 1, t, at, :] if c > 0 else west_halo[t]

        def from_east(c, t):
            return field[b, c + 1, t, at, :] if c < last else east_halo[t]

        totals = []
        for n, c in enumerate(group):
            total = None
            for t in range(tiles):
                if t == 1:
                    beside = jnp.where(lane_piece < cut_w, from_west(c, t), from_east(c, t))
                elif t == 2:
                    beside = from_east(c, t)
                elif t == 3:
                    beside = jnp.where(lane_piece < cut_e, from_east(c, t), from_west(c, t))
                else:
                    beside = from_west(c, t)
                if t < 2:
                    along = field[b, c, t, up, :]
                elif t == 2:
                    along = jnp.where(lane_piece < cut_y, field[b, c, t, up, :], field[b, c, t, down, :])
                else:
                    along = field[b, c, t, down, :]
                advected = (
                    keep_x[t, span, :] * field[b, c, t, at, :]
                    + push_x[t, span, :] * beside
                    + push_y[t, 0:1, :] * along
                )
                field[1 - b, c, t, at, :] = advected
                rounded[n * piece : (n + 1) * piece, t * LANES : (t + 1) * LANES] = advected.astype(
                    jnp.bfloat16
                )
                total = advected if total is None else total + advected
            energy = jnp.sum(total, axis=1, keepdims=True) * mean_of
            sea_here = scale[c, span, :]
            totals.append(grow[c, span, :] - (time_step * dissipation) * energy * sea_here)
        size = len(group) * piece
        transfer = jnp.dot(rounded[0:size, :], weights[...], preferred_element_type=jnp.float32)
        for n, c in enumerate(group):
            sea_here = time_step * scale[c, span, :]
            for t in range(tiles):
                moved = transfer[n * piece : (n + 1) * piece, t * LANES : (t + 1) * LANES]
                value = totals[n] * field[1 - b, c, t, at, :] + sea_here * moved
                if step < STEPS - 1:
                    field[1 - b, c, t, at, :] = value
                else:
                    w = width(t)
                    out_ref[c, span, t * LANES : t * LANES + w] = value[:, 0:w]

    heard = 2 + has_south.astype(jnp.int32) + has_north.astype(jnp.int32)
    pl.semaphore_wait(barrier, heard)

    def take_column(c):
        for t in range(tiles):
            w = width(t)
            field[0, c, t, PAD : PAD + rows, 0:w] = (
                staged[c, :, t * LANES : t * LANES + w] * scale[c, :, 0:w]
            )

    for c in edges:
        field[0, c, tiles - 1, PAD : PAD + rows, :] = jnp.zeros((rows, LANES), jnp.float32)
    for c in edges:
        loads[c].wait()
    for c in inner:
        loads[c].start()
    weight_load.start()
    for c in edges:
        take_column(c)
    for k in range(CHUNKS):
        send_lon(0, k)

    for copy in small[1:]:
        copy.wait()
    forcing = wind_ref[...] * (1.0 - ice_ref[...].astype(jnp.float32))
    growth = jnp.transpose(sea * (1.0 + time_step * forcing))
    for c in range(columns):
        grow[c] = jnp.broadcast_to(growth[:, c : c + 1], (rows, LANES))
    row = lax.broadcasted_iota(jnp.int32, (rows, LANES), 0) + lat * rows
    latitude = (-60.0 + 120.0 * (row.astype(jnp.float32) + 0.5) / (rows * lats)) * (math.pi / 180.0)
    inverse = 1.0 / jnp.cos(latitude)
    for t in range(tiles):
        number = (lane + t * LANES).astype(jnp.float32)
        direction = jnp.floor((number + 0.5) * (1.0 / freqs))
        freq = number - direction * freqs
        speed = jnp.zeros((8, LANES), jnp.float32)
        for f in range(freqs):
            speed = jnp.where(freq == f, speed_ref[f], speed)
        inside = (lane + t * LANES) < bins
        theta = (direction + 0.5) * (2.0 * math.pi / DIRS)
        along_y = jnp.where(inside, jnp.abs(0.45 * jnp.sin(theta) * speed), 0.0)
        along_x = jnp.where(inside, jnp.abs(0.225 * jnp.cos(theta) * speed), 0.0)
        push_y[t] = along_y
        along_x = along_x[0:1] * inverse
        push_x[t] = along_x
        keep_x[t] = 1.0 - along_x - along_y[0:1]

    zero_row = jnp.zeros((1, LANES), jnp.float32)
    for c in range(columns):
        for t in range(tiles):
            for b in range(2):
                field[b, c, t, PAD - 1 : PAD, :] = zero_row
                field[b, c, t, PAD + rows : PAD + rows + 1, :] = zero_row
        if c in inner:
            field[0, c, tiles - 1, PAD : PAD + rows, :] = jnp.zeros((rows, LANES), jnp.float32)

    for c in inner:
        loads[c].wait()
        take_column(c)
    send_north(0)
    send_south(0)

    weight_load.wait()
    weights[...] = jnp.zeros_like(weights)
    weights[0:bins, 0:bins] = raw_weights[...]

    for step in range(STEPS - 1):
        for k in range(CHUNKS):
            if k == 0:
                take_south(step)
            if k == CHUNKS - 1:
                take_north(step)
            for side in range(2):
                lon_copy(step, side, k).wait_recv()
            advance(step, k, edges)
            send_lon(step + 1, k)
            advance(step, k, inner)
            if k == 0:
                send_south(step + 1)
            if k == CHUNKS - 1:
                send_north(step + 1)
    take_south(STEPS - 1)
    take_north(STEPS - 1)
    for k in range(CHUNKS):
        advance(STEPS - 1, k, inner)
    for k in range(CHUNKS):
        for side in range(2):
            lon_copy(STEPS - 1, side, k).wait_recv()
        advance(STEPS - 1, k, edges)
    for step in range(STEPS):
        for k in range(CHUNKS):
            for side in range(2):
                lon_copy(step, side, k).wait_send()

        @pl.when(has_north)
        def _():
            lat_copy(step, 0).wait_send()

        @pl.when(has_south)
        def _():
            lat_copy(step, 1).wait_send()


def on_device(spectrum, sea_mask, ice_flags, wind_forcing, group_speed, coupling):
    columns, rows, bins = spectrum.shape
    tiles = -(-bins // LANES)
    wide = tiles * LANES
    piece = rows // CHUNKS
    hbm = pl.BlockSpec(memory_space=pltpu.HBM)
    operands = (group_speed, sea_mask, ice_flags, wind_forcing, spectrum, coupling)
    f32 = jnp.float32
    lon_buffer = pltpu.VMEM((STEPS, CHUNKS, 41, LANES), f32)
    lat_buffer = pltpu.VMEM((STEPS, 3, columns, LANES), f32)
    return pl.pallas_call(
        functools.partial(kernel, group_speed.shape[0]),
        out_shape=jax.ShapeDtypeStruct(spectrum.shape, spectrum.dtype),
        in_specs=[hbm] * 6,
        out_specs=pl.BlockSpec(memory_space=pltpu.VMEM),
        scratch_shapes=[
            pltpu.SMEM(group_speed.shape, f32),
            pltpu.VMEM((columns, rows), jnp.int32),
            pltpu.VMEM((columns, rows), jnp.int32),
            pltpu.VMEM((columns, rows), f32),
            pltpu.VMEM((2, columns, tiles, rows + 2 * PAD, LANES), f32),
            pltpu.VMEM((columns, rows, bins), f32),
            pltpu.VMEM((wide, wide), jnp.bfloat16),
            pltpu.VMEM((bins, bins), jnp.bfloat16),
            pltpu.VMEM(((columns - 2) * piece, wide), jnp.bfloat16),
            pltpu.VMEM((tiles, rows, LANES), f32),
            pltpu.VMEM((tiles, rows, LANES), f32),
            pltpu.VMEM((tiles, 8, LANES), f32),
            pltpu.VMEM((columns, rows, LANES), f32),
            pltpu.VMEM((columns, rows, LANES), f32),
            lon_buffer, lon_buffer, lon_buffer, lon_buffer,
            lat_buffer, lat_buffer, lat_buffer, lat_buffer,
            pltpu.SemaphoreType.DMA((columns,)),
            pltpu.SemaphoreType.DMA((4,)),
            pltpu.SemaphoreType.DMA,
            pltpu.SemaphoreType.DMA((STEPS, 2, CHUNKS)),
            pltpu.SemaphoreType.DMA((STEPS, 2, CHUNKS)),
            pltpu.SemaphoreType.DMA((STEPS, 2)),
            pltpu.SemaphoreType.DMA((STEPS, 2)),
        ],
        compiler_params=pltpu.CompilerParams(
            collective_id=0, has_side_effects=True, vmem_limit_bytes=32 * 1024 * 1024
        ),
    )(*(pltpu.with_memory_space_constraint(x, pltpu.HBM) for x in operands))


def solution(mesh):
    placed = (P("lon", "lat", None), P("lon", "lat"), P("lon", "lat"), P("lon", "lat"), P(), P())
    return jax.shard_map(
        on_device, mesh=mesh, in_specs=placed, out_specs=P("lon", "lat", None), check_vma=False
    )
```

```python
import functools
import math

import jax
import jax.numpy as jnp
from jax import lax
from jax.experimental import pallas as pl
from jax.experimental.pallas import tpu as pltpu
from jax.sharding import PartitionSpec as P

DIRS = 36
STEPS = 4
LANES = 128
PAD = 8
CHUNKS = 4
MESH = pl.DeviceIdType.MESH

time_step = 0.2
dissipation = 0.5


def kernel(
    freqs, speed_hbm, sea_hbm, ice_hbm, wind_hbm, spectrum_ref, coupling_ref, out_ref,
    speed_ref, sea_ref, ice_ref, wind_ref,
    field, staged, weights, raw_weights, rounded, keep_x, push_x, push_y, grow, scale,
    east_out, east_in, west_out, west_in, north_out, north_in, south_out, south_in,
    load_sem, small_sem, weight_sem, lon_send, lon_recv, lat_send, lat_recv,
):
    columns, rows, bins = staged.shape
    tiles = field.shape[2]
    piece = rows // CHUNKS
    mean_of = 1.0 / bins
    quarter, half, late = DIRS // 4 * freqs, DIRS // 2 * freqs, DIRS * 3 // 4 * freqs
    cut_w, cut_y, cut_e = quarter - LANES, half - 2 * LANES, late - 3 * LANES
    late_w = LANES - cut_e
    tail = bins - (tiles - 1) * LANES

    lon, lat = lax.axis_index("lon"), lax.axis_index("lat")
    lons, lats = lax.axis_size("lon"), lax.axis_size("lat")
    east, west = lax.rem(lon + 1, lons), lax.rem(lon + lons - 1, lons)
    has_south, has_north = lat > 0, lat < lats - 1

    def width(t):
        return LANES if t < tiles - 1 else tail

    last = columns - 1
    edges, inner = [0, last], list(range(1, last))
    loads = [
        pltpu.make_async_copy(spectrum_ref.at[c], staged.at[c], load_sem.at[c])
        for c in range(columns)
    ]
    weight_load = pltpu.make_async_copy(coupling_ref, raw_weights, weight_sem)
    small = [
        pltpu.make_async_copy(source, target, small_sem.at[n])
        for n, (source, target) in enumerate(
            ((sea_hbm, sea_ref), (speed_hbm, speed_ref), (ice_hbm, ice_ref), (wind_hbm, wind_ref))
        )
    ]
    for copy in small:
        copy.start()
    for c in edges:
        loads[c].start()

    barrier = pltpu.get_barrier_semaphore()
    pl.semaphore_signal(barrier, inc=1, device_id=(east, lat), device_id_type=MESH)
    pl.semaphore_signal(barrier, inc=1, device_id=(west, lat), device_id_type=MESH)

    @pl.when(has_south)
    def _():
        pl.semaphore_signal(barrier, inc=1, device_id=(lon, lat - 1), device_id_type=MESH)

    @pl.when(has_north)
    def _():
        pl.semaphore_signal(barrier, inc=1, device_id=(lon, lat + 1), device_id_type=MESH)

    small[0].wait()
    sea = sea_ref[...].astype(jnp.float32)
    sea_rows = jnp.transpose(sea)
    for c in range(columns):
        scale[c] = jnp.broadcast_to(sea_rows[:, c : c + 1], (rows, LANES))

    lane = lax.broadcasted_iota(jnp.int32, (8, LANES), 1)
    lane_piece = lax.broadcasted_iota(jnp.int32, (piece, LANES), 1)
    lane_eight = lax.broadcasted_iota(jnp.int32, (8, LANES), 1)
    row_eight = lax.broadcasted_iota(jnp.int32, (8, LANES), 0)
    own_low = lane_eight // 4 == row_eight + 1
    own_high = lane_eight // 4 == row_eight + 9
    low_half = lane_eight < LANES // 2

    def turn(value, by):
        return pltpu.roll(value, by % LANES, 1)

    def gather_rest(upper, lower, start):
        base = (4 - start) % LANES
        up = pltpu.roll(upper, base, 1, stride=4, stride_axis=0)
        down = pltpu.roll(lower, base + 32, 1, stride=4, stride_axis=0)
        spread = jnp.where(own_low, up, 0.0) + jnp.where(own_high, down, 0.0)
        return jnp.sum(spread, axis=0, keepdims=True)

    def spread_rest(line, start):
        line = jnp.broadcast_to(line, (8, LANES))
        halves = []
        for part in range(2):
            value = turn(line, start - 4 - 32 * part)
            for i in range(1, 8):
                value = jnp.where(row_eight == i, turn(line, start - 4 - 4 * i - 32 * part), value)
            halves.append(value)
        return halves

    def lon_copy(step, side, k):
        out_buf, in_buf, to = ((east_out, west_in, east), (west_out, east_in, west))[side]
        return pltpu.make_async_remote_copy(
            src_ref=out_buf.at[step, k],
            dst_ref=in_buf.at[step, k],
            send_sem=lon_send.at[step, side, k],
            recv_sem=lon_recv.at[step, side, k],
            device_id=(to, lat),
            device_id_type=MESH,
        )

    def lat_copy(step, side):
        out_buf, in_buf, to = ((north_out, south_in, lat + 1), (south_out, north_in, lat - 1))[side]
        return pltpu.make_async_remote_copy(
            src_ref=out_buf.at[step],
            dst_ref=in_buf.at[step],
            send_sem=lat_send.at[step, side],
            recv_sem=lat_recv.at[step, side],
            device_id=(lon, to),
            device_id_type=MESH,
        )

    def send_lon(step, k):
        b = step % 2
        at = slice(PAD + k * piece, PAD + (k + 1) * piece)
        buffer = east_out.at[step, k]
        buffer[0:16, :] = field[b, last, 0, at, :]
        buffer[16:32, :] = field[b, last, 4, at, :]
        ends = []
        for part in range(2):
            rows_at = slice(at.start + 8 * part, at.start + 8 * part + 8)
            move, offset = late_w + 64 * part, lane_eight - 64 * part
            value = jnp.where(
                offset < cut_w + late_w,
                turn(field[b, last, 1, rows_at, :], move),
                turn(field[b, last, 5, rows_at, :], move + cut_w),
            )
            ends.append(
                jnp.where(offset < late_w, turn(field[b, last, 3, rows_at, :], move), value)
            )
        buffer[32:40, :] = jnp.where(low_half, ends[0], ends[1])
        buffer[40:41, :] = gather_rest(
            field[b, last, 5, at.start : at.start + 8, :], field[b, last, 5, at.start + 8 : at.stop, :],
            64 - late_w - cut_w,
        )
        buffer = west_out.at[step, k]
        first_part = field[b, 0, 1, at, :]
        buffer[0:16, :] = field[b, 0, 2, at, :]
        buffer[16:32, :] = jnp.where(lane_piece < cut_e, field[b, 0, 3, at, :], first_part)
        buffer[32:40, :] = jnp.where(
            low_half, turn(first_part[0:8], -cut_w), turn(first_part[8:16], 64 - cut_w)
        )
        buffer[40:41, :] = gather_rest(first_part[0:8], first_part[8:16], 64 + cut_w)
        lon_copy(step, 0, k).start()
        lon_copy(step, 1, k).start()

    def send_north(step):
        b = step % 2
        low = lane[0:1] < cut_y
        edge = slice(PAD + rows - 1, PAD + rows)
        for c in range(columns):
            for i in range(3):
                north_out[step, i, c : c + 1, :] = field[b, c, i, edge, :]

        @pl.when(has_north)
        def _():
            lat_copy(step, 0).start()

    def send_south(step):
        b = step % 2
        low = lane[0:1] < cut_y
        edge = slice(PAD, PAD + 1)
        for c in range(columns):
            south_out[step, 0, c : c + 1, :] = jnp.where(
                low, field[b, c, 5, edge, :], field[b, c, 2, edge, :]
            )
            for i in range(1, 3):
                south_out[step, i, c : c + 1, :] = field[b, c, i + 2, edge, :]

        @pl.when(has_south)
        def _():
            lat_copy(step, 1).start()

    def take_south(step):
        b = step % 2

        @pl.when(has_south)
        def _():
            lat_copy(step, 0).wait_recv()
            for c in range(columns):
                for i in range(3):
                    field[b, c, i, PAD - 1 : PAD, :] = south_in[step, i, c : c + 1, :]

    def take_north(step):
        b = step % 2
        edge = slice(PAD + rows, PAD + rows + 1)

        @pl.when(has_north)
        def _():
            lat_copy(step, 1).wait_recv()
            for c in range(columns):
                for i, t in ((0, 2), (1, 3), (2, 4), (0, 5)):
                    field[b, c, t, edge, :] = north_in[step, i, c : c + 1, :]

    def advance(step, k, group, count=1):
        deep = count * piece
        lane_deep = lax.broadcasted_iota(jnp.int32, (deep, LANES), 1)
        b = step % 2
        at = slice(PAD + k * piece, PAD + (k + count) * piece)
        up = slice(at.start - 1, at.stop - 1)
        down = slice(at.start + 1, at.stop + 1)
        span = slice(k * piece, (k + count) * piece)
        if 0 in group:
            buffer = west_in.at[step, k]
            main, inside = buffer[32:40, :], 64 - late_w - cut_w
            rest = spread_rest(buffer[40:41, :], inside)
            shared = jnp.concatenate([turn(main, -late_w), turn(main, 64 - late_w)], axis=0)
            ends = [
                jnp.where(lane_eight < inside, turn(main, 64 * part + inside - 64), rest[part])
                for part in range(2)
            ]
            west_halo = {
                0: buffer[0:16, :],
                1: shared,
                3: shared,
                4: buffer[16:32, :],
                5: jnp.concatenate(ends, axis=0),
            }
        if last in group:
            buffer = east_in.at[step, k]
            main, shared = buffer[32:40, :], buffer[16:32, :]
            rest = spread_rest(buffer[40:41, :], 64 + cut_w)
            moved = [
                jnp.where(lane_eight < 64 + cut_w, turn(main, cut_w - 64 * part), rest[part])
                for part in range(2)
            ]
            moved = jnp.concatenate(moved, axis=0)
            east_halo = {
                1: jnp.where(lane_deep < cut_e, moved, shared), 2: buffer[0:16, :], 3: shared
            }

        def from_west(c, t):
            return field[b, c - 1, t, at, :] if c > 0 else west_halo[t]

        def from_east(c, t):
            return field[b, c + 1, t, at, :] if c < last else east_halo[t]

        totals = []
        for n, c in enumerate(group):
            total = None
            for t in range(tiles):
                if t == 1:
                    beside = jnp.where(lane_deep < cut_w, from_west(c, t), from_east(c, t))
                elif t == 2:
                    beside = from_east(c, t)
                elif t == 3:
                    beside = jnp.where(lane_deep < cut_e, from_east(c, t), from_west(c, t))
                else:
                    beside = from_west(c, t)
                if t < 2:
                    along = field[b, c, t, up, :]
                elif t == 2:
                    along = jnp.where(lane_deep < cut_y, field[b, c, t, up, :], field[b, c, t, down, :])
                else:
                    along = field[b, c, t, down, :]
                advected = (
                    keep_x[t, span, :] * field[b, c, t, at, :]
                    + push_x[t, span, :] * beside
                    + push_y[t, 0:1, :] * along
                )
                field[1 - b, c, t, at, :] = advected
                rounded[n * deep : (n + 1) * deep, t * LANES : (t + 1) * LANES] = advected.astype(
                    jnp.bfloat16
                )
                total = advected if total is None else total + advected
            energy = jnp.sum(total, axis=1, keepdims=True) * mean_of
            sea_here = scale[c, span, :]
            totals.append(grow[c, span, :] - (time_step * dissipation) * energy * sea_here)
        size = len(group) * deep
        transfer = jnp.dot(rounded[0:size, :], weights[...], preferred_element_type=jnp.float32)
        for n, c in enumerate(group):
            sea_here = time_step * scale[c, span, :]
            for t in range(tiles):
                moved = transfer[n * deep : (n + 1) * deep, t * LANES : (t + 1) * LANES]
                value = totals[n] * field[1 - b, c, t, at, :] + sea_here * moved
                if step < STEPS - 1:
                    field[1 - b, c, t, at, :] = value
                else:
                    w = width(t)
                    out_ref[c, span, t * LANES : t * LANES + w] = value[:, 0:w]

    heard = 2 + has_south.astype(jnp.int32) + has_north.astype(jnp.int32)
    pl.semaphore_wait(barrier, heard)

    def take_column(c):
        for t in range(tiles):
            w = width(t)
            field[0, c, t, PAD : PAD + rows, 0:w] = (
                staged[c, :, t * LANES : t * LANES + w] * scale[c, :, 0:w]
            )

    for c in edges:
        field[0, c, tiles - 1, PAD : PAD + rows, :] = jnp.zeros((rows, LANES), jnp.float32)
    for c in edges:
        loads[c].wait()
    for c in inner:
        loads[c].start()
    weight_load.start()
    for c in edges:
        take_column(c)
    send_order = list(range(1, CHUNKS - 1)) + [0, CHUNKS - 1]
    for k in send_order:
        send_lon(0, k)

    for copy in small[1:]:
        copy.wait()
    forcing = wind_ref[...] * (1.0 - ice_ref[...].astype(jnp.float32))
    growth = jnp.transpose(sea * (1.0 + time_step * forcing))
    for c in range(columns):
        grow[c] = jnp.broadcast_to(growth[:, c : c + 1], (rows, LANES))
    row = lax.broadcasted_iota(jnp.int32, (rows, LANES), 0) + lat * rows
    latitude = (-60.0 + 120.0 * (row.astype(jnp.float32) + 0.5) / (rows * lats)) * (math.pi / 180.0)
    inverse = 1.0 / jnp.cos(latitude)
    for t in range(tiles):
        number = (lane + t * LANES).astype(jnp.float32)
        direction = jnp.floor((number + 0.5) * (1.0 / freqs))
        freq = number - direction * freqs
        speed = jnp.zeros((8, LANES), jnp.float32)
        for f in range(freqs):
            speed = jnp.where(freq == f, speed_ref[f], speed)
        inside = (lane + t * LANES) < bins
        theta = (direction + 0.5) * (2.0 * math.pi / DIRS)
        along_y = jnp.where(inside, jnp.abs(0.45 * jnp.sin(theta) * speed), 0.0)
        along_x = jnp.where(inside, jnp.abs(0.225 * jnp.cos(theta) * speed), 0.0)
        push_y[t] = along_y
        along_x = along_x[0:1] * inverse
        push_x[t] = along_x
        keep_x[t] = 1.0 - along_x - along_y[0:1]

    zero_row = jnp.zeros((1, LANES), jnp.float32)
    for c in range(columns):
        for t in range(tiles):
            for b in range(2):
                field[b, c, t, PAD - 1 : PAD, :] = zero_row
                field[b, c, t, PAD + rows : PAD + rows + 1, :] = zero_row
        if c in inner:
            field[0, c, tiles - 1, PAD : PAD + rows, :] = jnp.zeros((rows, LANES), jnp.float32)

    for c in inner:
        loads[c].wait()
        take_column(c)
    send_north(0)
    send_south(0)

    weight_load.wait()
    weights[...] = jnp.zeros_like(weights)
    weights[0:bins, 0:bins] = raw_weights[...]

    for step in range(STEPS):
        final = step == STEPS - 1

        def rim(k):
            for side in range(2):
                lon_copy(step, side, k).wait_recv()
            advance(step, k, edges)
            if not final:
                send_lon(step + 1, k)

        if final:
            advance(step, 1, inner, CHUNKS - 2)
        else:
            for k in range(1, CHUNKS - 1):
                rim(k)
            advance(step, 1, inner, CHUNKS - 2)
        take_south(step)
        if not final:
            rim(0)
        advance(step, 0, inner)
        if not final:
            send_south(step + 1)
        take_north(step)
        if not final:
            rim(CHUNKS - 1)
        advance(step, CHUNKS - 1, inner)
        if not final:
            send_north(step + 1)
        else:
            for k in send_order:
                rim(k)
    for step in range(STEPS):
        for k in range(CHUNKS):
            for side in range(2):
                lon_copy(step, side, k).wait_send()

        @pl.when(has_north)
        def _():
            lat_copy(step, 0).wait_send()

        @pl.when(has_south)
        def _():
            lat_copy(step, 1).wait_send()


def on_device(spectrum, sea_mask, ice_flags, wind_forcing, group_speed, coupling):
    columns, rows, bins = spectrum.shape
    tiles = -(-bins // LANES)
    wide = tiles * LANES
    piece = rows // CHUNKS
    hbm = pl.BlockSpec(memory_space=pltpu.HBM)
    operands = (group_speed, sea_mask, ice_flags, wind_forcing, spectrum, coupling)
    f32 = jnp.float32
    lon_buffer = pltpu.VMEM((STEPS, CHUNKS, 41, LANES), f32)
    lat_buffer = pltpu.VMEM((STEPS, 3, columns, LANES), f32)
    return pl.pallas_call(
        functools.partial(kernel, group_speed.shape[0]),
        out_shape=jax.ShapeDtypeStruct(spectrum.shape, spectrum.dtype),
        in_specs=[hbm] * 6,
        out_specs=pl.BlockSpec(memory_space=pltpu.VMEM),
        scratch_shapes=[
            pltpu.SMEM(group_speed.shape, f32),
            pltpu.VMEM((columns, rows), jnp.int32),
            pltpu.VMEM((columns, rows), jnp.int32),
            pltpu.VMEM((columns, rows), f32),
            pltpu.VMEM((2, columns, tiles, rows + 2 * PAD, LANES), f32),
            pltpu.VMEM((columns, rows, bins), f32),
            pltpu.VMEM((wide, wide), jnp.bfloat16),
            pltpu.VMEM((bins, bins), jnp.bfloat16),
            pltpu.VMEM(((columns - 2) * piece * 2, wide), jnp.bfloat16),
            pltpu.VMEM((tiles, rows, LANES), f32),
            pltpu.VMEM((tiles, rows, LANES), f32),
            pltpu.VMEM((tiles, 8, LANES), f32),
            pltpu.VMEM((columns, rows, LANES), f32),
            pltpu.VMEM((columns, rows, LANES), f32),
            lon_buffer, lon_buffer, lon_buffer, lon_buffer,
            lat_buffer, lat_buffer, lat_buffer, lat_buffer,
            pltpu.SemaphoreType.DMA((columns,)),
            pltpu.SemaphoreType.DMA((4,)),
            pltpu.SemaphoreType.DMA,
            pltpu.SemaphoreType.DMA((STEPS, 2, CHUNKS)),
            pltpu.SemaphoreType.DMA((STEPS, 2, CHUNKS)),
            pltpu.SemaphoreType.DMA((STEPS, 2)),
            pltpu.SemaphoreType.DMA((STEPS, 2)),
        ],
        compiler_params=pltpu.CompilerParams(
            collective_id=0, has_side_effects=True, vmem_limit_bytes=32 * 1024 * 1024
        ),
    )(*(pltpu.with_memory_space_constraint(x, pltpu.HBM) for x in operands))


def solution(mesh):
    placed = (P("lon", "lat", None), P("lon", "lat"), P("lon", "lat"), P("lon", "lat"), P(), P())
    return jax.shard_map(
        on_device, mesh=mesh, in_specs=placed, out_specs=P("lon", "lat", None), check_vma=False
    )
```
